8 devices in a mesh: rep: 1 (over z), mp: 2 (over y), tb: 2 (over x), ta: 2 (over core).
Axes of the slice: x: 2, y: 2, z: 1, core: 2. Of those that a mesh axis runs over, the one named last changes fastest.
Arguments:
- x_in: bfloat16 [8192, 2048], P(('rep', 'ta', 'tb'), 'mp')
- seg_ids: int32 [8192], P(('rep', 'ta', 'tb'))
- tok_pos: int32 [8192], P(('rep', 'ta', 'tb'))
- w_query: bfloat16 [2, 2048, 2048], P(None, ('ta', 'tb'), 'mp')
- w_key: bfloat16 [2, 2048, 128], P(None, ('ta', 'tb'))
- w_value: bfloat16 [2, 2048, 128], P(None, ('ta', 'tb'))
- w_gate: bfloat16 [2, 2048, 8192], P(None, ('ta', 'tb'), 'mp')
- w_up: bfloat16 [2, 2048, 8192], P(None, ('ta', 'tb'), 'mp')
- w_out: bfloat16 [2, 2048, 2048], P(None, 'mp', ('ta', 'tb'))
- w_down: bfloat16 [2, 8192, 2048], P(None, 'mp', ('ta', 'tb'))
- norm_gain: bfloat16 [2, 2048], replicated
Outputs:
- output: float32 [8192, 2048], P(('rep', 'ta', 'tb'), 'mp')
All inputs are finite; a program needn't handle non-finite values.
Results may differ from the reference program's by a relative error of at most 0.012314.
Values are sent between devices in bfloat16 or wider.
A program may use at most 1 GiB of HBM per device.

```python
import jax
import jax.numpy as jnp
from jax import lax

EMBED_DIM = 2048
NUM_HEADS = 16
HEAD_DIM = 128
FFN_DIM = 8192
BLOCK_TOKENS = 2048
TOKEN_BLOCKS = 4
LAYER_COUNT = 2

TOKENS = BLOCK_TOKENS * TOKEN_BLOCKS
UNIT_TOKENS = BLOCK_TOKENS // 8
NORM_EPS = 1e-6
ROPE_BASE = 10000.0


def request_layout(lay_key):
    key_full, key_cut, key_dens, key_bits = jax.random.split(lay_key, 4)
    full_block = jax.random.randint(key_full, (), 0, TOKEN_BLOCKS)
    cut_block = (full_block + 1 + jax.random.randint(key_cut, (), 0, TOKEN_BLOCKS - 1)) % TOKEN_BLOCKS
    block_ids = jnp.arange(TOKEN_BLOCKS)[:, None]
    density = jax.random.randint(key_dens, (TOKEN_BLOCKS, 1), 0, 9)
    density = jnp.where(block_ids == full_block, 0, density)
    density = jnp.where(block_ids == cut_block, 8, density)
    cut_draw = jax.random.randint(key_bits, (TOKEN_BLOCKS, 8), 0, 8)
    unit_ids = jnp.arange(8)[None, :]
    starts = ((cut_draw < density) | (unit_ids == 0)).astype(jnp.int32).reshape(-1)
    unit_seg = jnp.cumsum(starts) - 1
    unit_first = lax.cummax(jnp.arange(TOKEN_BLOCKS * 8) * starts, axis=0)
    seg_ids = jnp.repeat(unit_seg, UNIT_TOKENS, total_repeat_length=TOKENS)
    first_tok = jnp.repeat(unit_first, UNIT_TOKENS, total_repeat_length=TOKENS) * UNIT_TOKENS
    tok_pos = jnp.arange(TOKENS) - first_tok
    return seg_ids.astype(jnp.int32), tok_pos.astype(jnp.int32)


def draw_weight(wkey, shape, fan_in, scale_mult):
    base = jax.random.normal(wkey, (LAYER_COUNT,) + shape, jnp.float32)
    return (base * (scale_mult * fan_in ** -0.5)).astype(jnp.bfloat16)


def setup_inputs(seed: int = 0, part: int = 0) -> dict:
    part_key = jax.random.fold_in(jax.random.key(seed), part)
    key_x, key_lay = jax.random.split(part_key)
    wkeys = jax.random.split(jax.random.key(seed + 1), 8)
    seg_ids, tok_pos = request_layout(key_lay)
    head_width = NUM_HEADS * HEAD_DIM
    x_in = jax.random.normal(key_x, (TOKENS, EMBED_DIM), jnp.float32).astype(jnp.bfloat16)
    norm_vals = 1.0 + 0.3 * jax.random.normal(wkeys[7], (LAYER_COUNT, EMBED_DIM), jnp.float32)
    return {
        "x_in": x_in,
        "seg_ids": seg_ids,
        "tok_pos": tok_pos,
        "w_query": draw_weight(wkeys[0], (EMBED_DIM, head_width), EMBED_DIM, 2.0),
        "w_key": draw_weight(wkeys[1], (EMBED_DIM, HEAD_DIM), EMBED_DIM, 1.0),
        "w_value": draw_weight(wkeys[2], (EMBED_DIM, HEAD_DIM), EMBED_DIM, 1.0),
        "w_gate": draw_weight(wkeys[3], (EMBED_DIM, FFN_DIM), EMBED_DIM, 1.0),
        "w_up": draw_weight(wkeys[4], (EMBED_DIM, FFN_DIM), EMBED_DIM, 1.0),
        "w_out": draw_weight(wkeys[5], (head_width, EMBED_DIM), head_width, 2.0),
        "w_down": draw_weight(wkeys[6], (FFN_DIM, EMBED_DIM), FFN_DIM, 1.0),
        "norm_gain": norm_vals.astype(jnp.bfloat16),
    }


def rotary(vals, positions):
    half = HEAD_DIM // 2
    inv_freq = ROPE_BASE ** (-2.0 * jnp.arange(half, dtype=jnp.float32) / HEAD_DIM)
    angle = positions.astype(jnp.float32)[:, None, None] * inv_freq
    cos_a = jnp.cos(angle)
    sin_a = jnp.sin(angle)
    first = vals[..., :half]
    second = vals[..., half:]
    return jnp.concatenate([first * cos_a - second * sin_a, second * cos_a + first * sin_a], axis=-1)


def block_attention(blk_args):
    q_blk, k_blk, v_blk, seg_blk, pos_blk = blk_args
    allowed = (seg_blk[:, None] == seg_blk[None, :]) & (pos_blk[None, :] <= pos_blk[:, None])

    def one_head(q_head):
        scores = jnp.dot(q_head, k_blk.T, preferred_element_type=jnp.float32) * HEAD_DIM ** -0.5
        scores = jnp.where(allowed, scores, -jnp.inf)
        expo = jnp.exp(scores - jnp.max(scores, axis=-1, keepdims=True))
        probs = (expo / jnp.sum(expo, axis=-1, keepdims=True)).astype(jnp.bfloat16)
        return jnp.dot(probs, v_blk, preferred_element_type=jnp.float32).astype(jnp.bfloat16)

    heads_out = lax.map(one_head, jnp.moveaxis(q_blk, 1, 0))
    return jnp.moveaxis(heads_out, 0, 1)


def parallel_layer(resid, weights, seg_ids, tok_pos):
    w_query, w_key, w_value, w_gate, w_up, w_out, w_down, norm_gain = weights
    mean_sq = jnp.mean(jnp.square(resid), axis=-1, keepdims=True)
    h_act = (resid * lax.rsqrt(mean_sq + NORM_EPS) * norm_gain.astype(jnp.float32)).astype(jnp.bfloat16)
    q_all = jnp.dot(h_act, w_query, preferred_element_type=jnp.float32).reshape(TOKENS, NUM_HEADS, HEAD_DIM)
    q_all = rotary(q_all, tok_pos).astype(jnp.bfloat16)
    k_all = rotary(jnp.dot(h_act, w_key, preferred_element_type=jnp.float32)[:, None, :], tok_pos)[:, 0, :].astype(jnp.bfloat16)
    v_all = jnp.dot(h_act, w_value, preferred_element_type=jnp.float32).astype(jnp.bfloat16)
    gate = jnp.dot(h_act, w_gate, preferred_element_type=jnp.float32).astype(jnp.bfloat16)
    up_act = jnp.dot(h_act, w_up, preferred_element_type=jnp.float32).astype(jnp.bfloat16)
    mlp_act = (jax.nn.silu(gate.astype(jnp.float32)) * up_act.astype(jnp.float32)).astype(jnp.bfloat16)
    attn = lax.map(block_attention, (
        q_all.reshape(TOKEN_BLOCKS, BLOCK_TOKENS, NUM_HEADS, HEAD_DIM),
        k_all.reshape(TOKEN_BLOCKS, BLOCK_TOKENS, HEAD_DIM),
        v_all.reshape(TOKEN_BLOCKS, BLOCK_TOKENS, HEAD_DIM),
        seg_ids.reshape(TOKEN_BLOCKS, BLOCK_TOKENS),
        tok_pos.reshape(TOKEN_BLOCKS, BLOCK_TOKENS),
    ))
    attn = attn.reshape(TOKENS, NUM_HEADS * HEAD_DIM)
    branch = jnp.dot(attn, w_out, preferred_element_type=jnp.float32) + jnp.dot(mlp_act, w_down, preferred_element_type=jnp.float32)
    return resid + branch


def reference(x_in, seg_ids, tok_pos, w_query, w_key, w_value, w_gate, w_up, w_out, w_down, norm_gain):
    def layer_step(resid, weights):
        return parallel_layer(resid, weights, seg_ids, tok_pos), None

    y_out, unused = lax.scan(layer_step, x_in.astype(jnp.float32), (w_query, w_key, w_value, w_gate, w_up, w_out, w_down, norm_gain))
    return y_out
```

```python
import functools

import jax
import jax.numpy as jnp
from jax import lax
from jax.experimental import pallas as pl
from jax.experimental.pallas import tpu as pltpu
from jax.sharding import PartitionSpec as P

NORM_EPS = 1e-6
ROPE_BASE = 10000.0
TOKEN_AXES = ("rep", "ta", "tb")
TOKEN_PLANE = ("ta", "tb")
SWAP = [(0, 1), (1, 0)]
F32 = jnp.float32
BF16 = jnp.bfloat16
GU_CHUNKS = 4


def params(dims=1, mib=56):
    return pltpu.CompilerParams(
        dimension_semantics=("arbitrary",) * dims, vmem_limit_bytes=mib * 1024 * 1024)


def dot(a, b):
    return jnp.dot(a, b, preferred_element_type=F32)


ANY = pl.BlockSpec(memory_space=pl.ANY)
SMEM = pl.BlockSpec(memory_space=pltpu.SMEM)


def load_h(flag_ref, own_ref, oth_ref, hs, sem):
    same = flag_ref[0]

    @pl.when(same == 1)
    def _():
        first = pltpu.make_async_copy(own_ref, hs.at[0], sem.at[0])
        second = pltpu.make_async_copy(oth_ref, hs.at[1], sem.at[1])
        first.start()
        second.start()
        first.wait()
        second.wait()

    @pl.when(same == 0)
    def _():
        first = pltpu.make_async_copy(oth_ref, hs.at[0], sem.at[0])
        second = pltpu.make_async_copy(own_ref, hs.at[1], sem.at[1])
        first.start()
        second.start()
        first.wait()
        second.wait()


def norm_kernel(tb_ref, xo_ref, xt_ref, go_ref, gt_ref, ho_ref, ht_ref):
    half = xo_ref.shape[1] // 2
    xo = xo_ref[...].astype(F32)
    xt = xt_ref[...].astype(F32)
    width = 2 * xo_ref.shape[1]
    total = jnp.sum(xo * xo, axis=-1, keepdims=True) + jnp.sum(xt * xt, axis=-1, keepdims=True)
    scale = lax.rsqrt(total / width + NORM_EPS)
    ho = (xo * scale * go_ref[...]).astype(BF16)
    ht = (xt * scale * gt_ref[...]).astype(BF16)

    @pl.when(tb_ref[0] == 0)
    def _():
        ho_ref[...] = ho
        ht_ref[...] = ht

    @pl.when(tb_ref[0] == 1)
    def _():
        ho_ref[:, :half] = ho[:, half:]
        ho_ref[:, half:] = ho[:, :half]
        ht_ref[:, :half] = ht[:, half:]
        ht_ref[:, half:] = ht[:, :half]


def norm_first(tb, x_own, x_oth, gain_own, gain_oth):
    tokens, width = x_own.shape
    tile = 256
    blk = pl.BlockSpec((tile, width), lambda i: (i, 0))
    row = pl.BlockSpec((1, width), lambda i: (0, 0))
    out = jax.ShapeDtypeStruct((tokens, width), BF16)
    return pl.pallas_call(
        norm_kernel, grid=(tokens // tile,),
        in_specs=[SMEM, blk, blk, row, row], out_specs=[blk, blk], out_shape=[out, out],
        compiler_params=params(),
        cost_estimate=pl.CostEstimate(flops=10 * tokens * width * 2, bytes_accessed=tokens * width * 8, transcendentals=0),
        name="norm_first",
    )(tb, x_own, x_oth, gain_own, gain_oth)


def rotate(vals, cos, sin):
    half = vals.shape[1] // 2
    turned = jnp.concatenate([vals[:, half:], vals[:, :half]], axis=1)
    return vals * cos + turned * sin


def qkv_kernel(flag_ref, own_ref, oth_ref, w0, w1, w2, w3, cos_ref, sin_ref, q_ref, k_ref, v_ref, hs, sem):
    @pl.when(pl.program_id(0) == 0)
    def _():
        load_h(flag_ref, own_ref, oth_ref, hs, sem)

    tile = q_ref.shape[0]
    q_cols = q_ref.shape[1]
    rows = pl.ds(pl.multiple_of(pl.program_id(0) * tile, tile), tile)
    half = hs.shape[2] // 2
    ha = hs[0, rows, :]
    hb = hs[1, rows, :]
    cos = cos_ref[...]
    sin = sin_ref[...]
    for c in range(w0.shape[1] // 256):
        cols = slice(c * 256, c * 256 + 256)
        acc = dot(ha[:, :half], w0[:, cols]) + dot(ha[:, half:], w1[:, cols])
        acc = acc + dot(hb[:, :half], w2[:, cols]) + dot(hb[:, half:], w3[:, cols])
        if c * 256 < q_cols:
            q_ref[:, c * 256:c * 256 + 128] = rotate(acc[:, :128], cos, sin).astype(BF16)
            q_ref[:, c * 256 + 128:c * 256 + 256] = rotate(acc[:, 128:], cos, sin).astype(BF16)
        else:
            k_ref[...] = rotate(acc[:, :128], cos, sin).astype(BF16)
            v_ref[...] = acc[:, 128:].astype(BF16)


def qkv_proj(flag, h_own, h_oth, ws, cos, sin):
    tokens, width = h_own.shape
    cols = ws[0].shape[1]
    head = cos.shape[1]
    q_cols = cols - 2 * head
    tile = 256
    wspec = pl.BlockSpec(ws[0].shape, lambda i: (0, 0))
    tab = pl.BlockSpec((tile, head), lambda i: (i, 0))
    return pl.pallas_call(
        qkv_kernel, grid=(tokens // tile,),
        in_specs=[SMEM, ANY, ANY, wspec, wspec, wspec, wspec, tab, tab],
        out_specs=[pl.BlockSpec((tile, q_cols), lambda i: (i, 0)), tab, tab],
        out_shape=[jax.ShapeDtypeStruct((tokens, q_cols), BF16),
                   jax.ShapeDtypeStruct((tokens, head), BF16), jax.ShapeDtypeStruct((tokens, head), BF16)],
        scratch_shapes=[pltpu.VMEM((2, tokens, width), BF16), pltpu.SemaphoreType.DMA((2,))],
        compiler_params=params(),
        cost_estimate=pl.CostEstimate(flops=4 * tokens * width * cols, bytes_accessed=8 * tokens * width, transcendentals=0),
        name="qkv_proj",
    )(flag, h_own, h_oth, *ws, cos, sin)


def attn_kernel(tile0, scale, start_ref, q_ref, k_ref, v_ref, o_ref):
    tile = q_ref.shape[0]
    for i in range(k_ref.shape[0] // tile - tile0):
        @pl.when(pl.program_id(1) == i)
        def _(i=i):
            first = (tile0 + i) * tile
            q = q_ref[...]
            start = start_ref[...]
            dims = (((1,), (1,)), ((), ()))
            neg = -jnp.inf
            sd = lax.dot_general(q, k_ref[first:first + tile, :], dims, preferred_element_type=F32) * scale
            col = lax.broadcasted_iota(jnp.int32, sd.shape, 1)
            row = lax.broadcasted_iota(jnp.int32, sd.shape, 0)
            sd = jnp.where((col <= row) & (col + first >= start), sd, neg)
            top = jnp.max(sd, axis=-1, keepdims=True)
            if first:
                so = lax.dot_general(q, k_ref[:first, :], dims, preferred_element_type=F32) * scale
                colo = lax.broadcasted_iota(jnp.int32, so.shape, 1)
                so = jnp.where(colo >= start, so, neg)
                top = jnp.maximum(top, jnp.max(so, axis=-1, keepdims=True))
                eo = jnp.exp(so - top)
            ed = jnp.exp(sd - top)
            total = jnp.sum(ed, axis=-1, keepdims=True)
            if first:
                total = total + jnp.sum(eo, axis=-1, keepdims=True)
            inv = 1.0 / total
            out = dot((ed * inv).astype(BF16), v_ref[first:first + tile, :])
            if first:
                out = out + dot((eo * inv).astype(BF16), v_ref[:first, :])
            o_ref[...] = out.astype(BF16)


def attention(start, q, k, v):
    q_tokens, q_cols = q.shape
    keys, head = k.shape
    tile = 512
    tile0 = (keys - q_tokens) // tile
    full = pl.BlockSpec((keys, head), lambda h, i: (0, 0))
    blk = pl.BlockSpec((tile, head), lambda h, i: (i, h))
    return pl.pallas_call(
        functools.partial(attn_kernel, tile0, head ** -0.5), grid=(q_cols // head, q_tokens // tile),
        in_specs=[pl.BlockSpec((tile, 1), lambda h, i: (i, 0)), blk, full, full],
        out_specs=blk, out_shape=jax.ShapeDtypeStruct((q_tokens, q_cols), BF16),
        compiler_params=params(2),
        cost_estimate=pl.CostEstimate(flops=16 * q_tokens * q_cols * keys, bytes_accessed=4 * q_tokens * q_cols, transcendentals=0),
        name="attention",
    )(start, q, k, v)


def gu_kernel(flag_ref, own_ref, oth_ref, w0, w1, w2, w3, m_ref, hs, sem):
    @pl.when(pl.program_id(0) == 0)
    def _():
        load_h(flag_ref, own_ref, oth_ref, hs, sem)

    half = hs.shape[2] // 2
    tile = 512
    for t in range(m_ref.shape[0] // tile):
        rows = slice(t * tile, t * tile + tile)
        accs = []
        for j in range(2):
            acc = dot(hs[0, rows, :half], w0[j]) + dot(hs[0, rows, half:], w1[j])
            acc = acc + dot(hs[1, rows, :half], w2[j]) + dot(hs[1, rows, half:], w3[j])
            accs.append(acc.astype(BF16).astype(F32))
        gate, up = accs
        m_ref[rows, :] = (gate * jax.nn.sigmoid(gate) * up).astype(BF16)


def gate_up(flag, h_own, h_oth, ws):
    tokens, width = h_own.shape
    depth, cols = ws[0].shape[1:]
    ntile = 256
    wspec = pl.BlockSpec((2, depth, ntile), lambda i: (0, 0, i))
    return pl.pallas_call(
        gu_kernel, grid=(cols // ntile,),
        in_specs=[SMEM, ANY, ANY, wspec, wspec, wspec, wspec],
        out_specs=pl.BlockSpec((tokens, ntile), lambda i: (0, i)),
        out_shape=jax.ShapeDtypeStruct((tokens, cols), BF16),
        scratch_shapes=[pltpu.VMEM((2, tokens, width), BF16), pltpu.SemaphoreType.DMA((2,))],
        compiler_params=params(),
        cost_estimate=pl.CostEstimate(flops=8 * tokens * width * cols, bytes_accessed=8 * tokens * width, transcendentals=0),
        name="gate_up",
    )(flag, h_own, h_oth, *ws)


def out_kernel(pick, flag_ref, wa_ref, wb_ref, o_ref, m0, m1, m2, m3, y_ref, ws, sem):
    @pl.when(pl.program_id(0) == 0)
    def _():
        if pick:
            @pl.when(flag_ref[0] == 1)
            def _():
                copy = pltpu.make_async_copy(wa_ref, ws, sem.at[0])
                copy.start()
                copy.wait()

            @pl.when(flag_ref[0] == 0)
            def _():
                copy = pltpu.make_async_copy(wb_ref, ws, sem.at[0])
                copy.start()
                copy.wait()
        else:
            rows = wa_ref.shape[0]
            for j in range(2):
                @pl.when(flag_ref[0] == j)
                def _(j=j):
                    first = pltpu.make_async_copy(wa_ref, ws.at[pl.ds(j * rows, rows)], sem.at[0])
                    second = pltpu.make_async_copy(wb_ref, ws.at[pl.ds((1 - j) * rows, rows)], sem.at[1])
                    first.start()
                    second.start()
                    first.wait()
                    second.wait()

    step = o_ref.shape[1]
    acc = dot(o_ref[...], ws[:step, :])
    pos = step
    for m in (m0, m1, m2, m3):
        acc = acc + dot(m[...], ws[pos:pos + m.shape[1], :])
        pos += m.shape[1]
    y_ref[...] = acc


def out_proj(pick, flag, wa, wb, attn, ms, first, tokens):
    cols = wa.shape[1]
    depth = attn.shape[1] + sum(m.shape[1] for m in ms)
    tile = 256
    base = first // tile
    specs = [pl.BlockSpec((tile, a.shape[1]), lambda i: (base + i, 0)) for a in (attn, *ms)]
    return pl.pallas_call(
        functools.partial(out_kernel, pick), grid=(tokens // tile,),
        in_specs=[SMEM, ANY, ANY, *specs],
        out_specs=pl.BlockSpec((tile, cols), lambda i: (i, 0)),
        out_shape=jax.ShapeDtypeStruct((tokens, cols), F32),
        scratch_shapes=[pltpu.VMEM((depth, cols), BF16), pltpu.SemaphoreType.DMA((2,))],
        compiler_params=params(),
        cost_estimate=pl.CostEstimate(flops=2 * tokens * depth * cols, bytes_accessed=2 * depth * (tokens + cols), transcendentals=0),
        name="out_proj",
    )(flag, wa, wb, attn, *ms)


def move(name, val, axis):
    with jax.named_scope(name):
        return lax.ppermute(val, axis, SWAP)


def solution(mesh):
    def device_fn(x_blk, seg_ids, tok_pos, w_query, w_key, w_value, w_gate, w_up, w_out, w_down, norm_gain):
        tokens, e_half = x_blk.shape
        layers = w_query.shape[0]
        head = w_key.shape[2]
        ffn = w_gate.shape[2]
        chunk = ffn // GU_CHUNKS
        piece = e_half // 2
        ta, tb, mp = lax.axis_index("ta"), lax.axis_index("tb"), lax.axis_index("mp")
        same = ta == mp
        flag = same.astype(jnp.int32).reshape(1)
        not_flag = 1 - flag
        ta_flag = ta.astype(jnp.int32).reshape(1)
        tb_flag = tb.astype(jnp.int32).reshape(1)
        hrows = (w_out.shape[1] + w_down.shape[1]) // 2

        x_oth = move("py_x", x_blk, "mp")
        qkv_w, gu_w, out_loc, out_oth_x, out_own_x = [], [], [], [], []
        for layer in range(layers):
            def spread(tag, own):
                far = move(f"px_{tag}_{layer}", own, "tb")
                sib = move(f"pd_{tag}_{layer}", own, "ta")
                far_sib = move(f"pf_{tag}_{layer}", far, "ta")
                return own, far, sib, far_sib

            cat = jnp.concatenate([w_query[layer], w_key[layer], w_value[layer]], axis=1)
            qkv_w.append(spread("qkv", cat))
            chunks = []
            for c in range(GU_CHUNKS):
                cols = slice(c * chunk, (c + 1) * chunk)
                chunks.append(spread(f"gu{c}", jnp.stack([w_gate[layer, :, cols], w_up[layer, :, cols]])))
            gu_w.append(chunks)
            own = jnp.concatenate([w_out[layer], w_down[layer]], axis=0)
            sib = move(f"pd_out_{layer}", own, "ta")
            out_loc.append((own, sib))
            halves = []
            for tag, pred in (("oth", same), ("own", jnp.logical_not(same))):
                mine = lax.dynamic_slice_in_dim(own, ta * hrows, hrows, axis=0)
                theirs = lax.dynamic_slice_in_dim(sib, ta * hrows, hrows, axis=0)
                far = move(f"px_{tag}_{layer}", jnp.where(pred, theirs, mine), "tb")
                halves.append((far, move(f"pf_{tag}_{layer}", far, "ta")))
            out_oth_x.append(halves[0])
            out_own_x.append(halves[1])

        half_dim = head // 2
        inv_freq = ROPE_BASE ** (-2.0 * jnp.arange(half_dim, dtype=F32) / head)
        angle = tok_pos.astype(F32)[:, None] * inv_freq
        cos = jnp.concatenate([jnp.cos(angle)] * 2, axis=1)
        sin_half = jnp.sin(angle)
        sin = jnp.concatenate([-sin_half, sin_half], axis=1)
        start = (jnp.arange(tokens, dtype=jnp.int32) - tok_pos)[:, None]

        gains = norm_gain.astype(F32).reshape(layers, 2, 1, e_half)
        gain_own = lax.dynamic_index_in_dim(gains, mp, 1, keepdims=False)
        gain_oth = lax.dynamic_index_in_dim(gains, 1 - mp, 1, keepdims=False)

        def roles(val):
            return jnp.where(tb == 0, val, jnp.concatenate([val[..., piece:], val[..., :piece]], axis=-1))

        span = tokens // 2
        h_own, h_oth = norm_first(tb_flag, x_blk, x_oth, gain_own[0], gain_oth[0])
        resid = roles(x_blk)
        resid = [resid[p * span:(p + 1) * span].astype(F32) for p in range(2)]

        def branch(layer, attn, ms, part, first):
            args = (attn, ms, first, span)
            oth_loc = out_proj(True, not_flag, *out_loc[layer], *args)
            got_loc = move(f"py_loc{part}_{layer}", oth_loc, "mp")
            oth_x = out_proj(False, ta_flag, *out_oth_x[layer], *args)
            got_x = move(f"py_far{part}_{layer}", oth_x, "mp")
            own_loc = out_proj(True, flag, *out_loc[layer], *args)
            own_x = out_proj(False, ta_flag, *out_own_x[layer], *args)
            return jnp.concatenate([own_loc + got_loc, own_x + got_x], axis=1)

        q, k, v = qkv_proj(flag, h_own, h_oth, qkv_w[0], cos, sin)
        attn = attention(start, q, k, v)
        ms = [gate_up(flag, h_own, h_oth, w) for w in gu_w[0]]
        resid = [resid[p] + branch(0, attn, ms, p, p * span) for p in range(2)]

        gain1 = roles(gain_own[1])
        outs = []
        keys, vals = [], []
        for p in range(2):
            sq = jnp.sum(jnp.square(resid[p]), axis=-1)
            sq_oth = move(f"py_sq{p}", sq.reshape(8, span // 8), "mp").reshape(span)
            scale = lax.rsqrt((sq + sq_oth) / (2 * e_half) + NORM_EPS)[:, None]
            ho = (resid[p] * scale * gain1).astype(BF16)
            ht = move(f"py_h{p}", ho, "mp")
            rows = slice(p * span, (p + 1) * span)
            q, k, v = qkv_proj(flag, ho, ht, qkv_w[1], cos[rows], sin[rows])
            keys.append(k)
            vals.append(v)
            kk = jnp.concatenate(keys, axis=0) if p else k
            vv = jnp.concatenate(vals, axis=0) if p else v
            attn = attention(start[rows], q, kk, vv)
            ms = [gate_up(flag, ho, ht, w) for w in gu_w[1]]
            outs.append(resid[p] + branch(1, attn, ms, p, 0))
        return jnp.concatenate([roles(o) for o in outs], axis=0)

    weight_in = P(None, TOKEN_PLANE, "mp")
    kv_spec = P(None, TOKEN_PLANE, None)
    weight_out = P(None, "mp", TOKEN_PLANE)
    return jax.shard_map(
        device_fn,
        mesh=mesh,
        in_specs=(P(TOKEN_AXES, "mp"), P(TOKEN_AXES), P(TOKEN_AXES), weight_in, kv_spec, kv_spec, weight_in, weight_in, weight_out, weight_out, P()),
        out_specs=P(TOKEN_AXES, "mp"),
        check_vma=False,
    )
```

```python
import functools

import jax
import jax.numpy as jnp
from jax import lax
from jax.experimental import pallas as pl
from jax.experimental.pallas import tpu as pltpu
from jax.sharding import PartitionSpec as P


NORM_EPS = 1e-6
ROPE_BASE = 10000.0
TOKEN_AXES = ("rep", "ta", "tb")
TOKEN_PLANE = ("ta", "tb")
SWAP = [(0, 1), (1, 0)]
F32 = jnp.float32
BF16 = jnp.bfloat16
GU_CHUNKS = 4
PARTS = 2
ATTN_TILE = 512
GU_TILE = 512
ATTN_AT = ((0, 0), (0, 2))


def params(dims=1):
    return pltpu.CompilerParams(
        dimension_semantics=("arbitrary",) * dims, vmem_limit_bytes=66_000_000)


def dot(a, b):
    return jnp.dot(a, b, preferred_element_type=F32)


ANY = pl.BlockSpec(memory_space=pl.ANY)
SMEM = pl.BlockSpec(memory_space=pltpu.SMEM)


def cost(flops, bytes_accessed):
    return pl.CostEstimate(flops=int(flops), bytes_accessed=int(bytes_accessed), transcendentals=0)


def pick_halves(flag_ref, own_ref, oth_ref, hs, sem, act):
    width = own_ref.shape[1]
    for value, pair in ((1, (own_ref, oth_ref)), (0, (oth_ref, own_ref))):
        @pl.when(flag_ref[0] == value)
        def _(pair=pair):
            for j, ref in enumerate(pair):
                act(pltpu.make_async_copy(ref, hs.at[:, pl.ds(j * width, width)], sem.at[j]))


def start(copy):
    copy.start()


def wait(copy):
    copy.wait()


def norm_kernel(tb_ref, xo_ref, xt_ref, go_ref, gt_ref, ho_ref, ht_ref):
    half = xo_ref.shape[1] // 2
    xo = xo_ref[...].astype(F32)
    xt = xt_ref[...].astype(F32)
    width = 2 * xo_ref.shape[1]
    total = jnp.sum(xo * xo, axis=-1, keepdims=True) + jnp.sum(xt * xt, axis=-1, keepdims=True)
    scale = lax.rsqrt(total / width + NORM_EPS)
    ho = (xo * scale * go_ref[...]).astype(BF16)
    ht = (xt * scale * gt_ref[...]).astype(BF16)

    @pl.when(tb_ref[0] == 0)
    def _():
        ho_ref[...] = ho
        ht_ref[...] = ht

    @pl.when(tb_ref[0] == 1)
    def _():
        ho_ref[:, :half] = ho[:, half:]
        ho_ref[:, half:] = ho[:, :half]
        ht_ref[:, :half] = ht[:, half:]
        ht_ref[:, half:] = ht[:, :half]


def norm_first(tb, x_own, x_oth, gain_own, gain_oth, first):
    tokens, width = x_oth.shape
    tile = 256
    base = first // tile
    row = pl.BlockSpec((1, width), lambda i: (0, 0))
    blk = pl.BlockSpec((tile, width), lambda i: (i, 0))
    out = jax.ShapeDtypeStruct((tokens, width), BF16)
    return pl.pallas_call(
        norm_kernel, grid=(tokens // tile,),
        in_specs=[SMEM, pl.BlockSpec((tile, width), lambda i: (base + i, 0)), blk, row, row],
        out_specs=[blk, blk], out_shape=[out, out],
        compiler_params=params(), cost_estimate=cost(20 * tokens * width, 8 * tokens * width),
        name="norm_first",
    )(tb, x_own, x_oth, gain_own, gain_oth)


def rotate(vals, cos, sin):
    half = vals.shape[1] // 2
    turned = jnp.concatenate([vals[:, half:], vals[:, :half]], axis=1)
    return vals * cos + turned * sin


def qkv_kernel(flag_ref, own_ref, oth_ref, w0, w1, w2, w3, cos_ref, sin_ref, q_ref, k_ref, v_ref, hs, ws, hsem, wsem):
    depth = w0.shape[0]

    @pl.when(pl.program_id(0) == 0)
    def _():
        copies = [pltpu.make_async_copy(w, ws.at[pl.ds(j * depth, depth)], wsem.at[j]) for j, w in enumerate((w0, w1, w2, w3))]
        pick_halves(flag_ref, own_ref, oth_ref, hs, hsem, start)
        for copy in copies:
            copy.start()
        pick_halves(flag_ref, own_ref, oth_ref, hs, hsem, wait)
        for copy in copies:
            copy.wait()

    tile, q_cols = q_ref.shape
    rows = pl.ds(pl.multiple_of(pl.program_id(0) * tile, tile), tile)
    h = hs[rows, :]
    cos = cos_ref[...]
    sin = sin_ref[...]
    for c in range(ws.shape[1] // 256):
        acc = dot(h, ws[:, c * 256:c * 256 + 256])
        if c * 256 < q_cols:
            q_ref[:, c * 256:c * 256 + 128] = rotate(acc[:, :128], cos, sin).astype(BF16)
            q_ref[:, c * 256 + 128:c * 256 + 256] = rotate(acc[:, 128:], cos, sin).astype(BF16)
        else:
            k_ref[...] = rotate(acc[:, :128], cos, sin).astype(BF16)
            v_ref[...] = acc[:, 128:].astype(BF16)


def qkv_proj(flag, h_own, h_oth, ws, cos, sin):
    tokens, width = h_own.shape
    depth, cols = ws[0].shape
    head = cos.shape[1]
    q_cols = cols - 2 * head
    tile = 512
    tab = pl.BlockSpec((tile, head), lambda i: (i, 0))
    kv = jax.ShapeDtypeStruct((tokens, head), BF16)
    return pl.pallas_call(
        qkv_kernel, grid=(tokens // tile,),
        in_specs=[SMEM, ANY, ANY, ANY, ANY, ANY, ANY, tab, tab],
        out_specs=[pl.BlockSpec((tile, q_cols), lambda i: (i, 0)), tab, tab],
        out_shape=[jax.ShapeDtypeStruct((tokens, q_cols), BF16), kv, kv],
        scratch_shapes=[pltpu.VMEM((tokens, 2 * width), BF16), pltpu.VMEM((4 * depth, cols), BF16),
                        pltpu.SemaphoreType.DMA((2,)), pltpu.SemaphoreType.DMA((4,))],
        compiler_params=params(), cost_estimate=cost(4 * tokens * width * cols, 6 * tokens * width),
        name="qkv_proj",
    )(flag, h_own, h_oth, *ws, cos, sin)


def attn_kernel(tile0, scale, first_ref, q_ref, k_ref, v_ref, *refs):
    o_ref = refs[-1]
    tile = q_ref.shape[0]
    dims = (((1,), (1,)), ((), ()))
    rate = scale * 1.4426950408889634
    for i in range(k_ref.shape[0] // tile - tile0):
        @pl.when(pl.program_id(1) == i)
        def _(i=i):
            base = (tile0 + i) * tile
            q = q_ref[...]
            first = first_ref[...]
            sd = lax.dot_general(q, k_ref[base:base + tile, :], dims, preferred_element_type=F32)
            col = lax.broadcasted_iota(jnp.int32, sd.shape, 1)
            row = lax.broadcasted_iota(jnp.int32, sd.shape, 0)
            sd = jnp.where((col <= row) & (col + base >= first), sd, -jnp.inf)
            top = jnp.max(sd, axis=-1, keepdims=True)
            if base:
                so = lax.dot_general(q, k_ref[:base, :], dims, preferred_element_type=F32)
                colo = lax.broadcasted_iota(jnp.int32, so.shape, 1)
                so = jnp.where(colo >= first, so, -jnp.inf)
                top = jnp.maximum(top, jnp.max(so, axis=-1, keepdims=True))
                eo = jnp.exp2((so - top) * rate)
            ed = jnp.exp2((sd - top) * rate)
            total = jnp.sum(ed, axis=-1, keepdims=True)
            if base:
                total = total + jnp.sum(eo, axis=-1, keepdims=True)
            inv = 1.0 / total
            out = dot((ed * inv).astype(BF16), v_ref[base:base + tile, :])
            if base:
                out = out + dot((eo * inv).astype(BF16), v_ref[:base, :])
            o_ref[...] = out.astype(BF16)


def attention(first, q, k, v, act_cols, act):
    q_tokens, q_cols = q.shape
    keys, head = k.shape
    tile = ATTN_TILE
    tile0 = (keys - q_tokens) // tile
    full = pl.BlockSpec((keys, head), lambda h, i: (0, 0))
    blk = pl.BlockSpec((tile, head), lambda h, i: (i, h))
    return pl.pallas_call(
        functools.partial(attn_kernel, tile0, head ** -0.5), grid=(q_cols // head, q_tokens // tile),
        in_specs=[pl.BlockSpec((tile, 1), lambda h, i: (i, 0)), blk, full, full] + ([] if act is None else [ANY]),
        out_specs=blk, out_shape=jax.ShapeDtypeStruct((q_tokens, act_cols), BF16),
        input_output_aliases={} if act is None else {4: 0},
        compiler_params=params(2), cost_estimate=cost(16 * q_tokens * q_cols * keys, 4 * q_tokens * q_cols),
        name="attention",
    )(first, q, k, v, *([] if act is None else [act]))


def gu_kernel(flag_ref, own_ref, oth_ref, w0, w1, w2, w3, *refs):
    m_ref, hs, ws, hsem, wsem = refs[-5:]
    step = pl.program_id(0)
    steps = pl.num_programs(0)
    depth = w0.shape[1]
    ntile = m_ref.shape[1]

    def copies(n, slot):
        cols = pl.ds(pl.multiple_of(n * ntile, ntile), ntile)
        return [pltpu.make_async_copy(w.at[:, :, cols], ws.at[slot, :, pl.ds(j * depth, depth), :], wsem.at[slot, j])
                for j, w in enumerate((w0, w1, w2, w3))]

    @pl.when(step == 0)
    def _():
        for copy in copies(0, 0):
            copy.start()
        pick_halves(flag_ref, own_ref, oth_ref, hs, hsem, start)

    for parity in range(2):
        @pl.when((step + 1 < steps) & (lax.rem(step + 1, 2) == parity))
        def _(parity=parity):
            for copy in copies(step + 1, parity):
                copy.start()

    @pl.when(step == 0)
    def _():
        pick_halves(flag_ref, own_ref, oth_ref, hs, hsem, wait)

    for parity in range(2):
        @pl.when(lax.rem(step, 2) == parity)
        def _(parity=parity):
            for copy in copies(step, parity):
                copy.wait()

    slot = lax.rem(step, 2)
    tile = GU_TILE

    def body(t, carry):
        rows = pl.ds(pl.multiple_of(t * tile, tile), tile)
        h = hs[rows, :]
        gate = dot(h, ws[slot, 0]).astype(BF16).astype(F32)
        up = dot(h, ws[slot, 1]).astype(BF16).astype(F32)
        m_ref[rows, :] = (gate * jax.nn.sigmoid(gate) * up).astype(BF16)
        return carry

    lax.fori_loop(0, m_ref.shape[0] // tile, body, 0)


def gate_up(flag, h_own, h_oth, ws, act_cols, act, col):
    tokens, width = h_own.shape
    depth, cols = ws[0].shape[1:]
    ntile = 256
    base = col // ntile
    return pl.pallas_call(
        gu_kernel, grid=(cols // ntile,),
        in_specs=[SMEM] + [ANY] * (6 if act is None else 7),
        out_specs=pl.BlockSpec((tokens, ntile), lambda i: (0, base + i)),
        out_shape=jax.ShapeDtypeStruct((tokens, act_cols), BF16),
        scratch_shapes=[pltpu.VMEM((tokens, 2 * width), BF16), pltpu.VMEM((2, 2, 4 * depth, ntile), BF16),
                        pltpu.SemaphoreType.DMA((2,)), pltpu.SemaphoreType.DMA((2, 4))],
        input_output_aliases={} if act is None else {7: 0},
        compiler_params=params(), cost_estimate=cost(8 * tokens * width * cols, 6 * tokens * width),
        name="gate_up",
    )(flag, h_own, h_oth, *ws, *([] if act is None else [act]))


def out_kernel(near, add, pos_ref, a_ref, wa_ref, wb_ref, *refs):
    y_ref = refs[-1]
    k = pl.program_id(0)
    if near:
        use_a = pos_ref[0] == 1
    else:
        use_a = (k // (pl.num_programs(0) // 2)) == pos_ref[0]
    w = jnp.where(use_a, wa_ref[...], wb_ref[...])
    tile = 512
    for t in range(y_ref.shape[0] // tile):
        rows = slice(t * tile, t * tile + tile)
        prod = dot(a_ref[rows, :], w)

        @pl.when(k == 0)
        def _():
            y_ref[rows, :] = prod + refs[0][rows, :] if add else prod

        @pl.when(k > 0)
        def _():
            y_ref[rows, :] += prod


def out_proj(near, pos, wa, wb, act, resid=None):
    tokens, depth = act.shape
    cols = wa.shape[1]
    ktile = 1280
    steps = depth // ktile
    half = steps // 2
    if near:
        wspec_a = pl.BlockSpec((ktile, cols), lambda k, pos: (k * pos[0], 0))
        wspec_b = pl.BlockSpec((ktile, cols), lambda k, pos: (k * (1 - pos[0]), 0))
    else:
        wspec_a = pl.BlockSpec((ktile, cols), lambda k, pos: (jnp.clip(k - half * pos[0], 0, half - 1), 0))
        wspec_b = pl.BlockSpec((ktile, cols), lambda k, pos: (jnp.clip(k - half * (1 - pos[0]), 0, half - 1), 0))
    whole = pl.BlockSpec((tokens, cols), lambda k, pos: (0, 0))
    add = resid is not None
    return pl.pallas_call(
        functools.partial(out_kernel, near, add),
        grid_spec=pltpu.PrefetchScalarGridSpec(
            num_scalar_prefetch=1, grid=(steps,),
            in_specs=[pl.BlockSpec((tokens, ktile), lambda k, pos: (0, k)), wspec_a, wspec_b] + ([whole] if add else []),
            out_specs=whole),
        out_shape=jax.ShapeDtypeStruct((tokens, cols), F32),
        compiler_params=params(), cost_estimate=cost(2 * tokens * depth * cols, 2 * depth * (tokens + cols)),
        name="out_proj",
    )(pos, act, wa, wb, *([resid] if add else []))


def final_kernel(pos_ref, a_ref, b_ref, *refs):
    refs[-1][...] = a_ref[...] + b_ref[...]


def final_add(pos, own, got, part, shape, y):
    tokens, cols = own.shape
    tile = 256
    base = part * (tokens // tile)
    blk = pl.BlockSpec((tile, cols), lambda i, pos: (i, 0))
    args = (own, got) if y is None else (own, got, y)
    return pl.pallas_call(
        final_kernel,
        grid_spec=pltpu.PrefetchScalarGridSpec(
            num_scalar_prefetch=1, grid=(tokens // tile,),
            in_specs=[blk, blk] + ([] if y is None else [ANY]),
            out_specs=pl.BlockSpec((tile, cols), lambda i, pos: (base + i, pos[0]))),
        out_shape=jax.ShapeDtypeStruct(shape, F32),
        input_output_aliases={} if y is None else {3: 0},
        compiler_params=params(), cost_estimate=cost(tokens * cols, 12 * tokens * cols),
        name="final_add",
    )(pos, *args)


def move(val, axis):
    return lax.ppermute(val, axis, SWAP)


def solution(mesh):
    def device_fn(x_blk, seg_ids, tok_pos, w_query, w_key, w_value, w_gate, w_up, w_out, w_down, norm_gain):
        tokens, e_half = x_blk.shape
        layers = w_query.shape[0]
        head = w_key.shape[2]
        chunk = w_gate.shape[2] // GU_CHUNKS
        piece = e_half // 2
        ta, tb, mp = lax.axis_index("ta"), lax.axis_index("tb"), lax.axis_index("mp")
        same = ta == mp
        flag = same.astype(jnp.int32).reshape(1)
        not_flag = 1 - flag
        ta_flag = ta.astype(jnp.int32).reshape(1)
        tb_flag = tb.astype(jnp.int32).reshape(1)
        o_rows = w_out.shape[1]
        depth = o_rows + w_down.shape[1]
        hrows = depth // 2
        span = tokens // PARTS

        x_oth = [move(x_blk[p * span:(p + 1) * span], "mp") for p in range(PARTS)]
        qkv_w, gu_w, out_loc, out_far = [], [], [], []
        for layer in range(layers):
            def spread(own):
                far = move(own, "tb")
                sib = move(own, "ta")
                far_sib = move(far, "ta")
                return own, far, sib, far_sib

            qkv_w.append(spread(jnp.concatenate([w_query[layer], w_key[layer], w_value[layer]], axis=1)))
            chunks = []
            for c in range(GU_CHUNKS):
                cols = slice(c * chunk, (c + 1) * chunk)
                chunks.append(spread(jnp.stack([w_gate[layer, :, cols], w_up[layer, :, cols]])))
            gu_w.append(chunks)
            own = jnp.concatenate([w_out[layer], w_down[layer]], axis=0)
            sib = move(own, "ta")
            out_loc.append((own, sib))
            halves = []
            for pred in (same, jnp.logical_not(same)):
                mine = lax.dynamic_slice_in_dim(own, ta * hrows, hrows, axis=0)
                theirs = lax.dynamic_slice_in_dim(sib, ta * hrows, hrows, axis=0)
                far = move(jnp.where(pred, theirs, mine), "tb")
                halves.append((far, move(far, "ta")))
            out_far.append(halves)

        half_dim = head // 2
        inv_freq = ROPE_BASE ** (-2.0 * jnp.arange(half_dim, dtype=F32) / head)
        angle = tok_pos.astype(F32)[:, None] * inv_freq
        cos = jnp.concatenate([jnp.cos(angle)] * 2, axis=1)
        sin_half = jnp.sin(angle)
        sin = jnp.concatenate([-sin_half, sin_half], axis=1)
        first_key = (jnp.arange(tokens, dtype=jnp.int32) - tok_pos)[:, None]

        gains = norm_gain.astype(F32).reshape(layers, 2, 1, e_half)
        gain_own = lax.dynamic_index_in_dim(gains, mp, 1, keepdims=False)
        gain_oth = lax.dynamic_index_in_dim(gains, 1 - mp, 1, keepdims=False)

        def role(val, far):
            return lax.dynamic_slice_in_dim(val, (1 - tb if far else tb) * piece, piece, axis=1)

        parts = range(PARTS)
        rows = [slice(p * span, (p + 1) * span) for p in parts]
        resid = [[role(x_blk[rows[p]], far).astype(F32) for far in range(2)] for p in parts]
        h = [norm_first(tb_flag, x_blk, x_oth[p], gain_own[0], gain_oth[0], p * span) for p in parts]
        for layer in range(layers):
            if layer:
                h = []
                gain = [role(gain_own[layer], far) for far in range(2)]
                for p in parts:
                    if p:
                        vals = lax.optimization_barrier((own[p], got[p], h[p - 1][0]))
                        own[p], got[p] = vals[0], vals[1]
                    resid[p] = [own[p][far] + got[p][far] for far in range(2)]
                    sq = sum(jnp.sum(jnp.square(r), axis=-1) for r in resid[p])
                    sq_oth = move(sq.reshape(8, span // 8), "mp").reshape(span)
                    scale = lax.rsqrt((sq + sq_oth) / (2 * e_half) + NORM_EPS)[:, None]
                    ho = jnp.concatenate([(resid[p][far] * scale * gain[far]).astype(BF16) for far in range(2)], axis=1)
                    h.append((ho, move(ho, "mp")))
            keys, vals, acts = [], [], []
            for p in parts:
                q, k, v = qkv_proj(flag, *h[p], qkv_w[layer], cos[rows[p]], sin[rows[p]])
                keys.append(k)
                vals.append(v)
                kk = jnp.concatenate(keys, axis=0) if p else k
                vv = jnp.concatenate(vals, axis=0) if p else v
                act = None
                for c in range(GU_CHUNKS + 1):
                    if c == ATTN_AT[layer][p]:
                        act = attention(first_key[rows[p]], q, kk, vv, depth, act)
                    if c < GU_CHUNKS:
                        act = gate_up(flag, *h[p], gu_w[layer][c], depth, act, o_rows + c * chunk)
                acts.append(act)
            own, got = [[], []], [[], []]
            for p in parts:
                oth = out_proj(True, not_flag, *out_loc[layer], acts[p])
                got[p].append(move(oth, "mp"))
                oth = out_proj(False, ta_flag, *out_far[layer][0], acts[p])
                got[p].append(move(oth, "mp"))
                own[p].append(out_proj(True, flag, *out_loc[layer], acts[p], resid[p][0]))
                own[p].append(out_proj(False, ta_flag, *out_far[layer][1], acts[p], resid[p][1]))
        y = None
        for far, pos in ((0, tb_flag), (1, 1 - tb_flag)):
            for p in parts:
                y = final_add(pos, own[p][far], got[p][far], p, (tokens, e_half), y)
        return y

    weight_in = P(None, TOKEN_PLANE, "mp")
    kv_spec = P(None, TOKEN_PLANE, None)
    weight_out = P(None, "mp", TOKEN_PLANE)
    return jax.shard_map(
        device_fn,
        mesh=mesh,
        in_specs=(P(TOKEN_AXES, "mp"), P(TOKEN_AXES), P(TOKEN_AXES), weight_in, kv_spec, kv_spec, weight_in, weight_in, weight_out, weight_out, P()),
        out_specs=P(TOKEN_AXES, "mp"),
        check_vma=False,
    )
```
